32 devices in a mesh: row: 8 (over z, x), col: 4 (over y, core).
Axes of the slice: x: 2, y: 2, z: 4, core: 2. Of those that a mesh axis runs over, the one named last changes fastest.
Arguments:
- field: bfloat16 [32, 1024, 2048], P(None, 'row', 'col'), may hold values from -6 to 6
- solid_flags: int32 [32, 128, 128], P(None, 'row', 'col'), may hold values 0 or 1
- deriv_matrix: bfloat16 [2048, 2048], replicated, may hold values from -0.125 to 0.125
Outputs:
- filtered: bfloat16 [32, 1024, 2048], P('col', 'row')
- deriv_z: bfloat16 [32, 1024, 2048], P('col', 'row')
The draws below stay inside these ranges and needn't reach their ends.
Inputs may be any that keep to these rules, and one draw needn't show every extreme that they name: `solid_flags`: 1 marks a solid block, 0 a fluid one.
All inputs are finite; a program needn't handle non-finite values.
Results may differ from the reference program's by a relative error of at most 0.0058.
Values may be sent and summed in bfloat16 or wider, within the bound.
A program may use at most 128 MiB of HBM per device.

```python
import jax
import jax.numpy as jnp
from jax import lax

NZ = 2048
YBLK = 8
ZBLK = 16
NX = 32
NY = 1024


def plant(drawn, rng, least, high):
    spot = [jax.random.randint(jax.random.fold_in(rng, axis), (), 0, length) for axis, length in enumerate(drawn.shape)]
    longest = drawn.shape.index(max(drawn.shape))
    neighbour = spot[:longest] + [(spot[longest] + 1) % drawn.shape[longest]] + spot[longest + 1:]
    return drawn.at[tuple(spot)].set(least).at[tuple(neighbour)].set(high)


def level_of(stream_key, shape, split, smallest, top_value):
    gain = 1.0
    for axis_at, blocks in split:
        steps = jax.random.uniform(jax.random.fold_in(jax.random.fold_in(stream_key, 6), axis_at), (blocks,), jnp.float32, smallest / len(split), top_value / len(split))
        gain = gain * jnp.repeat(jnp.exp(steps), shape[axis_at] // blocks).reshape((-1,) + (1,) * (len(shape) - 1 - axis_at))
    return gain


def gaussian(stream_key, extent, scale, most, split=(), kind=jnp.bfloat16):
    values = jax.random.normal(stream_key, extent, jnp.float32) * scale
    if len(split) > 0:
        values = level_of(stream_key, extent, split, -0.22, 0.18) * values
    return jnp.clip(values, min=-most, max=most).astype(kind)


def setup_inputs(seed: int = 0) -> dict:
    keys = jax.random.split(jax.random.key(seed), 4)
    field = gaussian(keys[0], (NX, NY, NZ), 1.0, 6.0, ((1, 8), (2, 4)))
    solid_flags = plant((jax.random.randint(keys[1], (NX, NY // YBLK, NZ // ZBLK), 0, 4) < 1).astype(jnp.int32), jax.random.fold_in(keys[1], 1), 0, 1)
    deriv_matrix = gaussian(keys[2], (NZ, NZ), NZ ** -0.5, 0.125)
    return {"field": field, "solid_flags": solid_flags, "deriv_matrix": deriv_matrix}


filter_taps = ((-3, 1.0), (-2, -6.0), (-1, 15.0), (0, -20.0), (1, 15.0), (2, -6.0), (3, 1.0))


def smooth(values, axis):
    total = values
    for offset, tap in filter_taps:
        total = total + (tap / 64.0) * jnp.roll(values, -offset, axis)
    return total


def reference(field, solid_flags, deriv_matrix):
    def one_plane(inputs):
        plane, flags = inputs
        blocks = flags.astype(jnp.float32)
        nyb, nzb = blocks.shape
        solid = jnp.broadcast_to(blocks[:, None, :, None], (nyb, YBLK, nzb, ZBLK)).reshape(nyb * YBLK, nzb * ZBLK)
        masked = plane.astype(jnp.float32) * (1.0 - solid)
        yfilt = smooth(masked, 0).astype(jnp.bfloat16)
        filtered = smooth(yfilt.astype(jnp.float32), 1).astype(jnp.bfloat16)
        deriv = jnp.dot(filtered, deriv_matrix, preferred_element_type=jnp.float32).astype(jnp.bfloat16)
        return filtered, deriv

    filtered, deriv_z = lax.map(one_plane, (field, solid_flags))
    return filtered, deriv_z
```

```python
import functools

import jax
import jax.numpy as jnp
from jax import lax
from jax.experimental import pallas as pl
from jax.experimental.pallas import tpu as pltpu
from jax.sharding import PartitionSpec as P

MESH = pl.DeviceIdType.MESH
HALO = 16
PAD = 128
WIDE = 256
TAPS = ((-3, 1.0), (-2, -6.0), (-1, 15.0), (0, 44.0), (1, 15.0), (2, -6.0), (3, 1.0))


def band(shape, source_dim, source_shift):
    source = lax.broadcasted_iota(jnp.int32, shape, source_dim) - source_shift
    target = lax.broadcasted_iota(jnp.int32, shape, 1 - source_dim)
    offset = source - target
    taps = jnp.zeros(shape, jnp.float32)
    for at, tap in TAPS:
        taps = jnp.where(offset == at, tap / 64.0, taps)
    return taps.astype(jnp.bfloat16)


def spread(shape, block_dim, size):
    block = lax.broadcasted_iota(jnp.int32, shape, block_dim) * size
    cell = lax.broadcasted_iota(jnp.int32, shape, 1 - block_dim)
    return jnp.where((cell >= block) & (cell < block + size), 1.0, 0.0).astype(jnp.bfloat16)


def exchange(
    rows, cols, early,
    field, flags, matrix,
    filt, deriv, dense,
    raw, keep, ext, ysend, lines, wz,
    load_sem, flag_sem, matrix_sem, halo_send, halo_recv, line_send, line_recv, flag_buf,
):
    r = lax.axis_index("row")
    c = lax.axis_index("col")
    up, down = lax.rem(r + 1, rows), lax.rem(r + rows - 1, rows)
    steps, ny, full = filt.shape
    nx, _, zl = field.shape
    nyb, nzb = flags.shape[1:]
    half = cols // 2
    order = [half] + [k for k in range(1, cols) if k != half]

    def peer(k):
        return lax.rem(c + k, cols)

    def load(s, k):
        return pltpu.make_async_copy(field.at[peer(k) * steps + s], raw.at[s, k], load_sem.at[s, k])

    flag_copy = pltpu.make_async_copy(flags, flag_buf, flag_sem)
    flag_copy.start()

    def start_loads(s, carry):
        for k in range(cols):
            load(s, k).start()
        return carry

    lax.fori_loop(0, steps, start_loads, 0)
    matrix_copy = pltpu.make_async_copy(matrix, dense, matrix_sem)
    matrix_copy.start()

    barrier = pltpu.get_barrier_semaphore()
    for k in order:
        pl.semaphore_signal(barrier, inc=1, device_id=(r, peer(k)), device_id_type=MESH)
    for side in (up, down):
        pl.semaphore_signal(barrier, inc=1, device_id=(side, c), device_id_type=MESH)

    flag_copy.wait()
    fluid = (1 - flag_buf[...]).astype(jnp.float32).astype(jnp.bfloat16).reshape(nx * nyb, nzb)
    widen = spread((nzb, zl), 0, zl // nzb)
    keep[...] = (
        jnp.dot(fluid, widen, preferred_element_type=jnp.float32)
        .astype(jnp.bfloat16)
        .reshape(nx, nyb, zl)
    )
    tall = spread((ny, nyb), 1, ny // nyb)
    wy = band((ny, ny + 2 * HALO), 1, HALO)

    def mask(s):
        for k in range(cols):
            load(s, k).wait()
            cover = jnp.dot(tall, keep[peer(k) * steps + s], preferred_element_type=jnp.float32)
            ext[s, k, HALO:HALO + ny, :] = (raw[s, k].astype(jnp.float32) * cover).astype(jnp.bfloat16)

    def halos(s):
        return (
            pltpu.make_async_remote_copy(
                src_ref=ext.at[s, :, pl.ds(ny, HALO), :],
                dst_ref=ext.at[s, :, pl.ds(0, HALO), :],
                send_sem=halo_send.at[0, s], recv_sem=halo_recv.at[0, s],
                device_id=(up, c), device_id_type=MESH,
            ),
            pltpu.make_async_remote_copy(
                src_ref=ext.at[s, :, pl.ds(HALO, HALO), :],
                dst_ref=ext.at[s, :, pl.ds(ny + HALO, HALO), :],
                send_sem=halo_send.at[1, s], recv_sem=halo_recv.at[1, s],
                device_id=(down, c), device_id_type=MESH,
            ),
        )

    mine = pl.ds(pl.multiple_of(PAD + c * zl, 128), zl)

    def hand(s, k):
        return pltpu.make_async_remote_copy(
            src_ref=ysend.at[s, k],
            dst_ref=lines.at[s, :, mine],
            send_sem=line_send.at[s, k], recv_sem=line_recv.at[s, k],
            device_id=(r, peer(k)), device_id_type=MESH,
        )

    mask(0)
    pl.semaphore_wait(barrier, cols + 1)
    for copy in halos(0):
        copy.start()

    def produce(s, carry):
        @pl.when(s + 1 < steps)
        def _():
            mask(s + 1)
            for copy in halos(s + 1):
                copy.start()

        for copy in halos(s):
            copy.wait_recv()
        for k in order:
            ysend[s, k] = jnp.dot(wy, ext[s, k], preferred_element_type=jnp.float32).astype(jnp.bfloat16)
            hand(s, k).start()
        lines[s, :, mine] = jnp.dot(wy, ext[s, 0], preferred_element_type=jnp.float32).astype(jnp.bfloat16)
        return carry

    lax.fori_loop(0, steps, produce, 0)
    wz[...] = band((WIDE + 2 * PAD, WIDE), 0, PAD)
    matrix_copy.wait()

    def smooth(s):
        for k in order:
            hand(s, k).wait_recv()
        lines[s, :, 0:PAD] = lines[s, :, full:full + PAD]
        lines[s, :, full + PAD:full + 2 * PAD] = lines[s, :, PAD:2 * PAD]
        for j in range(0, full, WIDE):
            filt[s, :, j:j + WIDE] = jnp.dot(
                lines[s, :, j:j + WIDE + 2 * PAD], wz[...], preferred_element_type=jnp.float32
            ).astype(jnp.bfloat16)

    def consume(g, carry):
        smooth(2 * g)
        smooth(2 * g + 1)
        pair = filt[pl.ds(2 * g, 2)].reshape(2 * ny, full)
        for j in range(0, full, WIDE):
            deriv[pl.ds(2 * g, 2), :, j:j + WIDE] = (
                jnp.dot(pair, dense[:, j:j + WIDE], preferred_element_type=jnp.float32)
                .astype(jnp.bfloat16)
                .reshape(2, ny, WIDE)
            )
        return carry

    lax.fori_loop(0, early // 2, consume, 0)
    for s in range(early, steps):
        smooth(s)

    def drain(s, carry):
        for copy in halos(s):
            copy.wait_send()
        for k in order:
            hand(s, k).wait_send()
        return carry

    lax.fori_loop(0, steps, drain, 0)


def finish(early, filt, deriv, dense, filt_out, deriv_out, late, sems):
    steps, ny, full = filt.shape
    first = pltpu.make_async_copy(filt, filt_out, sems.at[0])
    first.start()
    second = pltpu.make_async_copy(deriv, deriv_out.at[pl.ds(0, early)], sems.at[1])
    second.start()
    count = steps - early
    rest = filt[early:steps].reshape(count * ny, full)
    thirds = []
    for j in range(0, full, WIDE):
        late[:, :, j:j + WIDE] = (
            jnp.dot(rest, dense[:, j:j + WIDE], preferred_element_type=jnp.float32)
            .astype(jnp.bfloat16)
            .reshape(count, ny, WIDE)
        )
        copy = pltpu.make_async_copy(
            late.at[:, :, pl.ds(j, WIDE)],
            deriv_out.at[pl.ds(early, count), :, pl.ds(j, WIDE)],
            sems.at[2 + j // WIDE],
        )
        copy.start()
        thirds.append(copy)
    first.wait()
    second.wait()
    for copy in thirds:
        copy.wait()


def shards(rows, cols, field, solid_flags, deriv_matrix):
    nx, ny, zl = field.shape
    full = deriv_matrix.shape[0]
    steps = nx // cols
    early = (steps - 1) // 2 * 2
    bf16 = jnp.bfloat16
    dma = pltpu.SemaphoreType.DMA
    hbm = pl.BlockSpec(memory_space=pl.ANY)
    vmem = pl.BlockSpec(memory_space=pltpu.VMEM)
    filt, deriv, dense = pl.pallas_call(
        functools.partial(exchange, rows, cols, early),
        out_shape=(
            pltpu.VMEM((steps, ny, full), bf16),
            pltpu.VMEM((early, ny, full), bf16),
            pltpu.VMEM((full, full), bf16),
        ),
        in_specs=[hbm] * 3,
        out_specs=(vmem,) * 3,
        scratch_shapes=[
            pltpu.VMEM((steps, cols, ny, zl), bf16),
            pltpu.VMEM((nx, solid_flags.shape[1], zl), bf16),
            pltpu.VMEM((steps, cols, ny + 2 * HALO, zl), bf16),
            pltpu.VMEM((steps, cols, ny, zl), bf16),
            pltpu.VMEM((steps, ny, full + 2 * PAD), bf16),
            pltpu.VMEM((WIDE + 2 * PAD, WIDE), bf16),
            dma((steps, cols)),
            dma,
            dma,
            dma((2, steps)),
            dma((2, steps)),
            dma((steps, cols)),
            dma((steps, cols)),
            pltpu.VMEM(solid_flags.shape, jnp.int32),
        ],
        compiler_params=pltpu.CompilerParams(
            collective_id=0, has_side_effects=True, vmem_limit_bytes=36 * 1024 * 1024
        ),
        name="exchange",
    )(field, solid_flags, deriv_matrix)
    return pl.pallas_call(
        functools.partial(finish, early),
        out_shape=(
            jax.ShapeDtypeStruct((steps, ny, full), bf16),
            jax.ShapeDtypeStruct((steps, ny, full), bf16),
        ),
        in_specs=[vmem] * 3,
        out_specs=(hbm, hbm),
        scratch_shapes=[
            pltpu.VMEM((steps - early, ny, full), bf16),
            dma((2 + full // WIDE,)),
        ],
        compiler_params=pltpu.CompilerParams(vmem_limit_bytes=8 * 1024 * 1024),
        name="finish",
    )(filt, deriv, dense)


def solution(mesh):
    in_specs = (P(None, "row", "col"), P(None, "row", "col"), P())
    out_specs = (P("col", "row", None), P("col", "row", None))
    rows, cols = mesh.shape["row"], mesh.shape["col"]
    return jax.shard_map(
        functools.partial(shards, rows, cols), mesh=mesh, in_specs=in_specs, out_specs=out_specs, check_vma=False
    )
```

```python
import functools

import jax
import jax.numpy as jnp
from jax import lax
from jax.experimental import pallas as pl
from jax.experimental.pallas import tpu as pltpu
from jax.sharding import PartitionSpec as P

MESH = pl.DeviceIdType.MESH
HALO = 16
PAD = 128
WIDE = 256
TAPS = ((-3, 1.0), (-2, -6.0), (-1, 15.0), (0, 44.0), (1, 15.0), (2, -6.0), (3, 1.0))


def band(shape, source_dim, source_shift):
    source = lax.broadcasted_iota(jnp.int32, shape, source_dim) - source_shift
    target = lax.broadcasted_iota(jnp.int32, shape, 1 - source_dim)
    offset = source - target
    taps = jnp.zeros(shape, jnp.float32)
    for at, tap in TAPS:
        taps = jnp.where(offset == at, tap / 64.0, taps)
    return taps.astype(jnp.bfloat16)


def spread(shape, block_dim, size):
    block = lax.broadcasted_iota(jnp.int32, shape, block_dim) * size
    cell = lax.broadcasted_iota(jnp.int32, shape, 1 - block_dim)
    return jnp.where((cell >= block) & (cell < block + size), 1.0, 0.0).astype(jnp.bfloat16)


def exchange(
    rows, cols, early,
    field, flags, matrix,
    filt, deriv, dense, lines, wz,
    raw, keep, ext, ysend,
    load_sem, flag_sem, matrix_sem, halo_send, halo_recv, line_send, line_recv,
    part_send, part_recv, flag_buf,
):
    r = lax.axis_index("row")
    c = lax.axis_index("col")
    up, down = lax.rem(r + 1, rows), lax.rem(r + rows - 1, rows)
    ny, full = filt.shape[1:]
    nx, _, zl = field.shape
    steps = nx // cols
    nyb, nzb = flags.shape[1:]
    half = cols // 2
    order = [half] + [k for k in range(1, cols) if k != half]

    def peer(k):
        return lax.rem(c + k, cols)

    def load(s, k):
        return pltpu.make_async_copy(field.at[peer(k) * steps + s], raw.at[s, k], load_sem.at[s, k])

    def start_loads(s, carry):
        for k in order + [0]:
            load(s, k).start()
        return carry

    barrier = pltpu.get_barrier_semaphore()
    for k in order:
        pl.semaphore_signal(barrier, inc=1, device_id=(r, peer(k)), device_id_type=MESH)
    for side in (up, down):
        pl.semaphore_signal(barrier, inc=1, device_id=(side, c), device_id_type=MESH)
    flag_copy = pltpu.make_async_copy(flags, flag_buf, flag_sem)
    flag_copy.start()
    lax.fori_loop(0, steps, start_loads, 0)
    matrix_copy = pltpu.make_async_copy(matrix, dense, matrix_sem)
    matrix_copy.start()

    flag_copy.wait()
    fluid = (1 - flag_buf[...]).astype(jnp.float32).astype(jnp.bfloat16).reshape(nx * nyb, nzb)
    widen = spread((nzb, zl), 0, zl // nzb)
    keep[...] = (
        jnp.dot(fluid, widen, preferred_element_type=jnp.float32)
        .astype(jnp.bfloat16)
        .reshape(nx, nyb, zl)
    )
    tall = spread((ny, nyb), 1, ny // nyb)
    inner = ny - 2 * HALO
    wy = band((ny, ny + 2 * HALO), 1, HALO)
    winner = band((inner, ny), 1, HALO)
    wedge = band((HALO, 3 * HALO), 1, HALO)
    cuts = (pl.ds(HALO, inner), pl.ds(0, HALO), pl.ds(ny - HALO, HALO))

    def mask(s):
        for k in order + [0]:
            load(s, k).wait()
            cover = jnp.dot(tall, keep[peer(k) * steps + s], preferred_element_type=jnp.float32)
            ext[s, k, HALO:HALO + ny, :] = (raw[s, k].astype(jnp.float32) * cover).astype(jnp.bfloat16)

    def halos(s):
        return (
            pltpu.make_async_remote_copy(
                src_ref=ext.at[s, :, pl.ds(ny, HALO), :],
                dst_ref=ext.at[s, :, pl.ds(0, HALO), :],
                send_sem=halo_send.at[0, s], recv_sem=halo_recv.at[0, s],
                device_id=(up, c), device_id_type=MESH,
            ),
            pltpu.make_async_remote_copy(
                src_ref=ext.at[s, :, pl.ds(HALO, HALO), :],
                dst_ref=ext.at[s, :, pl.ds(ny + HALO, HALO), :],
                send_sem=halo_send.at[1, s], recv_sem=halo_recv.at[1, s],
                device_id=(down, c), device_id_type=MESH,
            ),
        )

    mine = pl.ds(pl.multiple_of(PAD + c * zl, 128), zl)

    def hand(s, k):
        return pltpu.make_async_remote_copy(
            src_ref=ysend.at[s, k],
            dst_ref=lines.at[s, :, mine],
            send_sem=line_send.at[s, k], recv_sem=line_recv.at[s, k],
            device_id=(r, peer(k)), device_id_type=MESH,
        )

    def part(k, p):
        return pltpu.make_async_remote_copy(
            src_ref=ysend.at[0, k, cuts[p]],
            dst_ref=lines.at[0, cuts[p], mine],
            send_sem=part_send.at[p, k], recv_sem=part_recv.at[p, k],
            device_id=(r, peer(k)), device_id_type=MESH,
        )

    def apply(weights, block):
        return jnp.dot(weights, block, preferred_element_type=jnp.float32).astype(jnp.bfloat16)

    mask(0)
    pl.semaphore_wait(barrier, cols + 1)
    for copy in halos(0):
        copy.start()
    for k in order:
        ysend[0, k, HALO:HALO + inner] = apply(winner, ext[0, k, HALO:HALO + ny])
        part(k, 0).start()

    def advance(s):
        @pl.when(s + 1 < steps)
        def _():
            mask(s + 1)
            for copy in halos(s + 1):
                copy.start()

        for copy in halos(s):
            copy.wait_recv()

    advance(0)
    for k in order:
        ysend[0, k, 0:HALO] = apply(wedge, ext[0, k, 0:3 * HALO])
        part(k, 1).start()
        ysend[0, k, ny - HALO:ny] = apply(wedge, ext[0, k, ny - HALO:ny + 2 * HALO])
        part(k, 2).start()
    lines[0, :, mine] = apply(wy, ext[0, 0])

    def produce(s, carry):
        advance(s)
        for k in order:
            ysend[s, k] = apply(wy, ext[s, k])
            hand(s, k).start()
        lines[s, :, mine] = apply(wy, ext[s, 0])
        return carry

    lax.fori_loop(1, steps, produce, 0)
    wz[...] = band((WIDE + 2 * PAD, WIDE), 0, PAD)
    matrix_copy.wait()

    def arrive(s):
        for k in order:
            hand(s, k).wait_recv()

    def smooth(s):
        smooth_line(lines.at[s], wz, filt.at[s])

    def multiply(s, count):
        block = filt[pl.ds(s, count)].reshape(count * ny, full)
        for j in range(0, full, WIDE):
            deriv[pl.ds(s, count), :, j:j + WIDE] = apply(block, dense[:, j:j + WIDE]).reshape(count, ny, WIDE)

    def consume(g, carry):
        for s in (2 * g, 2 * g + 1):
            arrive(s)
            smooth(s)
        multiply(2 * g, 2)
        return carry

    for k in order:
        for p in range(3):
            part(k, p).wait_recv()
    smooth(0)
    arrive(1)
    smooth(1)
    multiply(0, 2)
    lax.fori_loop(1, early // 2, consume, 0)
    if early % 2:
        arrive(early - 1)
        smooth(early - 1)
        multiply(early - 1, 1)
    for copy in halos(0):
        copy.wait_send()
    for k in order:
        for p in range(3):
            part(k, p).wait_send()

    def drain(s, carry):
        for copy in halos(s):
            copy.wait_send()
        for k in order:
            hand(s, k).wait_send()
        return carry

    lax.fori_loop(1, steps, drain, 0)
    for s in range(early, steps):
        arrive(s)


def smooth_line(line, wz, out):
    full = out.shape[1]
    line[:, 0:PAD] = line[:, full:full + PAD]
    line[:, full + PAD:full + 2 * PAD] = line[:, PAD:2 * PAD]
    for j in range(0, full, WIDE):
        out[:, j:j + WIDE] = jnp.dot(
            line[:, j:j + WIDE + 2 * PAD], wz[...], preferred_element_type=jnp.float32
        ).astype(jnp.bfloat16)


def finish(filt, deriv, dense, lines, wz, filt_out, deriv_out, line, last, late, sems):
    early, ny, full = filt.shape
    copies = [
        pltpu.make_async_copy(filt, filt_out.at[pl.ds(0, early)], sems.at[0]),
        pltpu.make_async_copy(deriv, deriv_out.at[pl.ds(0, early)], sems.at[1]),
    ]
    for copy in copies:
        copy.start()
    line[...] = lines[early]
    smooth_line(line, wz, last)
    copies.append(pltpu.make_async_copy(last, filt_out.at[early], sems.at[2]))
    copies[-1].start()
    for j in range(0, full, WIDE):
        late[:, j:j + WIDE] = jnp.dot(
            last[...], dense[:, j:j + WIDE], preferred_element_type=jnp.float32
        ).astype(jnp.bfloat16)
        copies.append(
            pltpu.make_async_copy(
                late.at[:, pl.ds(j, WIDE)], deriv_out.at[early, :, pl.ds(j, WIDE)], sems.at[3 + j // WIDE]
            )
        )
        copies[-1].start()
    for copy in copies:
        copy.wait()


def shards(rows, cols, field, solid_flags, deriv_matrix):
    nx, ny, zl = field.shape
    full = deriv_matrix.shape[0]
    steps = nx // cols
    early = steps - 1
    bf16 = jnp.bfloat16
    dma = pltpu.SemaphoreType.DMA
    hbm = pl.BlockSpec(memory_space=pl.ANY)
    vmem = pl.BlockSpec(memory_space=pltpu.VMEM)
    held = pl.pallas_call(
        functools.partial(exchange, rows, cols, early),
        out_shape=(
            pltpu.VMEM((early, ny, full), bf16),
            pltpu.VMEM((early, ny, full), bf16),
            pltpu.VMEM((full, full), bf16),
            pltpu.VMEM((steps, ny, full + 2 * PAD), bf16),
            pltpu.VMEM((WIDE + 2 * PAD, WIDE), bf16),
        ),
        in_specs=[hbm] * 3,
        out_specs=(vmem,) * 5,
        scratch_shapes=[
            pltpu.VMEM((steps, cols, ny, zl), bf16),
            pltpu.VMEM((nx, solid_flags.shape[1], zl), bf16),
            pltpu.VMEM((steps, cols, ny + 2 * HALO, zl), bf16),
            pltpu.VMEM((steps, cols, ny, zl), bf16),
            dma((steps, cols)),
            dma,
            dma,
            dma((2, steps)),
            dma((2, steps)),
            dma((steps, cols)),
            dma((steps, cols)),
            dma((3, cols)),
            dma((3, cols)),
            pltpu.VMEM(solid_flags.shape, jnp.int32),
        ],
        compiler_params=pltpu.CompilerParams(
            collective_id=0, has_side_effects=True, vmem_limit_bytes=43 * 1024 * 1024
        ),
        name="exchange",
    )(field, solid_flags, deriv_matrix)
    return pl.pallas_call(
        finish,
        out_shape=(
            jax.ShapeDtypeStruct((steps, ny, full), bf16),
            jax.ShapeDtypeStruct((steps, ny, full), bf16),
        ),
        in_specs=[vmem] * 5,
        out_specs=(hbm, hbm),
        scratch_shapes=[
            pltpu.VMEM((ny, full + 2 * PAD), bf16),
            pltpu.VMEM((ny, full), bf16),
            pltpu.VMEM((ny, full), bf16),
            dma((3 + full // WIDE,)),
        ],
        compiler_params=pltpu.CompilerParams(vmem_limit_bytes=8 * 1024 * 1024),
        name="finish",
    )(*held)


def solution(mesh):
    in_specs = (P(None, "row", "col"), P(None, "row", "col"), P())
    out_specs = (P("col", "row", None), P("col", "row", None))
    rows, cols = mesh.shape["row"], mesh.shape["col"]
    return jax.shard_map(
        functools.partial(shards, rows, cols), mesh=mesh, in_specs=in_specs, out_specs=out_specs, check_vma=False
    )
```

```python
import functools

import jax
import jax.numpy as jnp
from jax import lax
from jax.experimental import pallas as pl
from jax.experimental.pallas import tpu as pltpu
from jax.sharding import PartitionSpec as P

MESH = pl.DeviceIdType.MESH
HALO = 16
PAD = 128
WIDE = 256
TAPS = ((-3, 1.0), (-2, -6.0), (-1, 15.0), (0, 44.0), (1, 15.0), (2, -6.0), (3, 1.0))


def band(shape, source_dim, source_shift):
    source = lax.broadcasted_iota(jnp.int32, shape, source_dim) - source_shift
    target = lax.broadcasted_iota(jnp.int32, shape, 1 - source_dim)
    offset = source - target
    taps = jnp.zeros(shape, jnp.float32)
    for at, tap in TAPS:
        taps = jnp.where(offset == at, tap / 64.0, taps)
    return taps.astype(jnp.bfloat16)


def spread(shape, block_dim, size):
    block = lax.broadcasted_iota(jnp.int32, shape, block_dim) * size
    cell = lax.broadcasted_iota(jnp.int32, shape, 1 - block_dim)
    return jnp.where((cell >= block) & (cell < block + size), 1.0, 0.0).astype(jnp.bfloat16)


def exchange(
    rows, cols, early,
    field, flags, matrix,
    filt, deriv, dense, lines, wz,
    raw, keep, ext, ysend,
    load_sem, flag_sem, matrix_sem, halo_send, halo_recv, line_send, line_recv,
    part_send, part_recv, flag_buf,
):
    r = lax.axis_index("row")
    c = lax.axis_index("col")
    up, down = lax.rem(r + 1, rows), lax.rem(r + rows - 1, rows)
    ny, full = filt.shape[1:]
    nx, _, zl = field.shape
    steps = nx // cols
    nyb, nzb = flags.shape[1:]
    half = cols // 2
    order = [half] + [k for k in range(1, cols) if k != half]

    def peer(k):
        return lax.rem(c + k, cols)

    def load(s, k):
        return pltpu.make_async_copy(field.at[peer(k) * steps + s], raw.at[s, k], load_sem.at[s, k])

    def start_loads(s, carry):
        for k in order + [0]:
            load(s, k).start()
        return carry

    barrier = pltpu.get_barrier_semaphore()
    for k in order:
        pl.semaphore_signal(barrier, inc=1, device_id=(r, peer(k)), device_id_type=MESH)
    for side in (up, down):
        pl.semaphore_signal(barrier, inc=1, device_id=(side, c), device_id_type=MESH)
    flag_copy = pltpu.make_async_copy(flags, flag_buf, flag_sem)
    flag_copy.start()
    start_loads(0, 0)
    matrix_copy = pltpu.make_async_copy(matrix, dense, matrix_sem)

    flag_copy.wait()
    fluid = (1 - flag_buf[...]).astype(jnp.float32).astype(jnp.bfloat16).reshape(nx * nyb, nzb)
    widen = spread((nzb, zl), 0, zl // nzb)
    keep[...] = (
        jnp.dot(fluid, widen, preferred_element_type=jnp.float32)
        .astype(jnp.bfloat16)
        .reshape(nx, nyb, zl)
    )
    tall = spread((ny, nyb), 1, ny // nyb)
    inner = ny - 2 * HALO
    wy = band((ny, ny + 2 * HALO), 1, HALO)
    winner = band((inner, ny), 1, HALO)
    wedge = band((HALO, 3 * HALO), 1, HALO)
    cuts = (pl.ds(HALO, inner), pl.ds(0, HALO), pl.ds(ny - HALO, HALO))

    def mask_line(s, k):
        load(s, k).wait()
        cover = jnp.dot(tall, keep[peer(k) * steps + s], preferred_element_type=jnp.float32)
        ext[s, k, HALO:HALO + ny, :] = (raw[s, k].astype(jnp.float32) * cover).astype(jnp.bfloat16)

    def mask(s):
        for k in order + [0]:
            mask_line(s, k)

    def halos(s):
        return (
            pltpu.make_async_remote_copy(
                src_ref=ext.at[s, :, pl.ds(ny, HALO), :],
                dst_ref=ext.at[s, :, pl.ds(0, HALO), :],
                send_sem=halo_send.at[0, s], recv_sem=halo_recv.at[0, s],
                device_id=(up, c), device_id_type=MESH,
            ),
            pltpu.make_async_remote_copy(
                src_ref=ext.at[s, :, pl.ds(HALO, HALO), :],
                dst_ref=ext.at[s, :, pl.ds(ny + HALO, HALO), :],
                send_sem=halo_send.at[1, s], recv_sem=halo_recv.at[1, s],
                device_id=(down, c), device_id_type=MESH,
            ),
        )

    mine = pl.ds(pl.multiple_of(PAD + c * zl, 128), zl)

    def hand(s, k):
        return pltpu.make_async_remote_copy(
            src_ref=ysend.at[s, k],
            dst_ref=lines.at[s, :, mine],
            send_sem=line_send.at[s, k], recv_sem=line_recv.at[s, k],
            device_id=(r, peer(k)), device_id_type=MESH,
        )

    def part(k, p):
        return pltpu.make_async_remote_copy(
            src_ref=ysend.at[0, k, cuts[p]],
            dst_ref=lines.at[0, cuts[p], mine],
            send_sem=part_send.at[p, k], recv_sem=part_recv.at[p, k],
            device_id=(r, peer(k)), device_id_type=MESH,
        )

    def apply(weights, block):
        return jnp.dot(weights, block, preferred_element_type=jnp.float32).astype(jnp.bfloat16)

    for i, k in enumerate(order):
        mask_line(0, k)
        ysend[0, k, HALO:HALO + inner] = apply(winner, ext[0, k, HALO:HALO + ny])
        if i == 0:
            pl.semaphore_wait(barrier, cols + 1)
        part(k, 0).start()
    mask_line(0, 0)
    for copy in halos(0):
        copy.start()
    lax.fori_loop(1, steps, start_loads, 0)
    matrix_copy.start()

    def advance(s):
        @pl.when(s + 1 < steps)
        def _():
            mask(s + 1)
            for copy in halos(s + 1):
                copy.start()

        for copy in halos(s):
            copy.wait_recv()

    advance(0)
    for k in order:
        ysend[0, k, 0:HALO] = apply(wedge, ext[0, k, 0:3 * HALO])
        part(k, 1).start()
        ysend[0, k, ny - HALO:ny] = apply(wedge, ext[0, k, ny - HALO:ny + 2 * HALO])
        part(k, 2).start()
    lines[0, :, mine] = apply(wy, ext[0, 0])

    def produce(s, carry):
        advance(s)
        for k in order:
            ysend[s, k] = apply(wy, ext[s, k])
            hand(s, k).start()
        lines[s, :, mine] = apply(wy, ext[s, 0])
        return carry

    lax.fori_loop(1, steps, produce, 0)
    wz[...] = band((WIDE + 2 * PAD, WIDE), 0, PAD)
    matrix_copy.wait()

    def arrive(s):
        for k in order:
            hand(s, k).wait_recv()

    def smooth(s):
        smooth_line(lines.at[s], wz, filt.at[s])

    def multiply(s, count):
        block = filt[pl.ds(s, count)].reshape(count * ny, full)
        for j in range(0, full, WIDE):
            deriv[pl.ds(s, count), :, j:j + WIDE] = apply(block, dense[:, j:j + WIDE]).reshape(count, ny, WIDE)

    def consume(g, carry):
        for s in (2 * g, 2 * g + 1):
            arrive(s)
            smooth(s)
        multiply(2 * g, 2)
        return carry

    for k in order:
        for p in range(3):
            part(k, p).wait_recv()
    smooth(0)
    arrive(1)
    smooth(1)
    multiply(0, 2)
    lax.fori_loop(1, early // 2, consume, 0)
    if early % 2:
        arrive(early - 1)
        smooth(early - 1)
        multiply(early - 1, 1)
    for copy in halos(0):
        copy.wait_send()
    for k in order:
        for p in range(3):
            part(k, p).wait_send()

    def drain(s, carry):
        for copy in halos(s):
            copy.wait_send()
        for k in order:
            hand(s, k).wait_send()
        return carry

    lax.fori_loop(1, steps, drain, 0)
    for s in range(early, steps):
        arrive(s)


def smooth_line(line, wz, out):
    full = out.shape[1]
    line[:, 0:PAD] = line[:, full:full + PAD]
    line[:, full + PAD:full + 2 * PAD] = line[:, PAD:2 * PAD]
    for j in range(0, full, WIDE):
        out[:, j:j + WIDE] = jnp.dot(
            line[:, j:j + WIDE + 2 * PAD], wz[...], preferred_element_type=jnp.float32
        ).astype(jnp.bfloat16)


def finish(filt, deriv, dense, lines, wz, filt_out, deriv_out, line, last, late, sems):
    early, ny, full = filt.shape
    copies = [
        pltpu.make_async_copy(filt, filt_out.at[pl.ds(0, early)], sems.at[0]),
        pltpu.make_async_copy(deriv, deriv_out.at[pl.ds(0, early)], sems.at[1]),
    ]
    for copy in copies:
        copy.start()
    line[...] = lines[early]
    smooth_line(line, wz, last)
    copies.append(pltpu.make_async_copy(last, filt_out.at[early], sems.at[2]))
    copies[-1].start()
    for j in range(0, full, WIDE):
        late[:, j:j + WIDE] = jnp.dot(
            last[...], dense[:, j:j + WIDE], preferred_element_type=jnp.float32
        ).astype(jnp.bfloat16)
        copies.append(
            pltpu.make_async_copy(
                late.at[:, pl.ds(j, WIDE)], deriv_out.at[early, :, pl.ds(j, WIDE)], sems.at[3 + j // WIDE]
            )
        )
        copies[-1].start()
    for copy in copies:
        copy.wait()


def shards(rows, cols, field, solid_flags, deriv_matrix):
    nx, ny, zl = field.shape
    full = deriv_matrix.shape[0]
    steps = nx // cols
    early = steps - 1
    bf16 = jnp.bfloat16
    dma = pltpu.SemaphoreType.DMA
    hbm = pl.BlockSpec(memory_space=pl.ANY)
    vmem = pl.BlockSpec(memory_space=pltpu.VMEM)
    held = pl.pallas_call(
        functools.partial(exchange, rows, cols, early),
        out_shape=(
            pltpu.VMEM((early, ny, full), bf16),
            pltpu.VMEM((early, ny, full), bf16),
            pltpu.VMEM((full, full), bf16),
            pltpu.VMEM((steps, ny, full + 2 * PAD), bf16),
            pltpu.VMEM((WIDE + 2 * PAD, WIDE), bf16),
        ),
        in_specs=[hbm] * 3,
        out_specs=(vmem,) * 5,
        scratch_shapes=[
            pltpu.VMEM((steps, cols, ny, zl), bf16),
            pltpu.VMEM((nx, solid_flags.shape[1], zl), bf16),
            pltpu.VMEM((steps, cols, ny + 2 * HALO, zl), bf16),
            pltpu.VMEM((steps, cols, ny, zl), bf16),
            dma((steps, cols)),
            dma,
            dma,
            dma((2, steps)),
            dma((2, steps)),
            dma((steps, cols)),
            dma((steps, cols)),
            dma((3, cols)),
            dma((3, cols)),
            pltpu.VMEM(solid_flags.shape, jnp.int32),
        ],
        compiler_params=pltpu.CompilerParams(
            collective_id=0, has_side_effects=True, vmem_limit_bytes=43 * 1024 * 1024
        ),
        name="exchange",
    )(field, solid_flags, deriv_matrix)
    return pl.pallas_call(
        finish,
        out_shape=(
            jax.ShapeDtypeStruct((steps, ny, full), bf16),
            jax.ShapeDtypeStruct((steps, ny, full), bf16),
        ),
        in_specs=[vmem] * 5,
        out_specs=(hbm, hbm),
        scratch_shapes=[
            pltpu.VMEM((ny, full + 2 * PAD), bf16),
            pltpu.VMEM((ny, full), bf16),
            pltpu.VMEM((ny, full), bf16),
            dma((3 + full // WIDE,)),
        ],
        compiler_params=pltpu.CompilerParams(vmem_limit_bytes=8 * 1024 * 1024),
        name="finish",
    )(*held)


def solution(mesh):
    in_specs = (P(None, "row", "col"), P(None, "row", "col"), P())
    out_specs = (P("col", "row", None), P("col", "row", None))
    rows, cols = mesh.shape["row"], mesh.shape["col"]
    return jax.shard_map(
        functools.partial(shards, rows, cols), mesh=mesh, in_specs=in_specs, out_specs=out_specs, check_vma=False
    )
```
